256 devices in a mesh: dp: 2 (over x_lo), expert: 128 (over y, z, x_hi, core).
Axes of the slice: x: 4 (x_hi: 2, x_lo: 2; x = x_hi * 2 + x_lo), y: 4, z: 8, core: 2. Of those that a mesh axis runs over, the one named last changes fastest.
Arguments:
- tokens: bfloat16 [256, 256, 1280], P(('dp', 'expert')), may hold values from -12 to 12
- router: bfloat16 [1280, 128], replicated, may hold values from -3 to 3
- w_in: bfloat16 [128, 1280, 5120], P('expert', None, 'dp'), may hold values from -0.15625 to 0.15625
- b_in: bfloat16 [128, 5120], P('expert'), may hold values from -3 to 3
- w_out: bfloat16 [128, 5120, 1280], P('expert', 'dp'), may hold values from -0.078125 to 0.078125
- b_out: bfloat16 [128, 1280], P('expert'), may hold values from -3 to 3
Outputs:
- mixed: bfloat16 [256, 256, 1280], P(('dp', 'expert'))
The draws below stay inside these ranges and needn't reach their ends.
All inputs are finite; a program needn't handle non-finite values.
Results may differ from the reference program's by a relative error of at most 0.014.
Values may be sent and summed in bfloat16 or wider, within the bound.
No kernel may reach another device: no remote copies, remote signals or barrier semaphores. Data moves between devices by JAX's collectives and lax.ppermute only.
A program may use at most 64 MiB of HBM per device.

```python
import math
import jax
import jax.numpy as jnp
from jax import lax

D = 1280
HID = 5120
M = 256
EXPERTS = 128
IMAGES = 256


def image_tokens(base, index):
    image_key = jax.random.fold_in(base, index)
    values = jnp.clip(jax.random.normal(jax.random.fold_in(image_key, 1), (M, D), jnp.float32), -6.0, 6.0)
    return values


def draw_tokens(key, part):
    base = jax.random.fold_in(key, 11)
    stacked = jax.vmap(lambda index: image_tokens(base, index))(jnp.arange(IMAGES))
    return stacked.astype(jnp.bfloat16)


def draw_router(key, part):
    values = jax.random.normal(jax.random.fold_in(key, 12), (D, EXPERTS), jnp.float32) * (2.5 / math.sqrt(D))
    values = jnp.clip(values, -0.5, 0.5)
    return values.astype(jnp.bfloat16)


def shard_levels(key, dims, cuts, low, top_value):
    def one(dim, parts):
        draws = jax.random.uniform(jax.random.fold_in(jax.random.fold_in(key, 6), dim), (parts,), jnp.float32, low / len(cuts), top_value / len(cuts))
        return jnp.repeat(jnp.exp(draws), dims[dim] // parts).reshape((-1,) + (1,) * (len(dims) - dim - 1))

    gain = one(*cuts[0])
    for cut in cuts[1:]:
        gain = gain * one(*cut)
    return gain


def bell_draw(stream_key, dims, deviation, reach, cuts=(), dtype=jnp.bfloat16):
    factor_of = shard_levels(stream_key, dims, cuts, -0.22, 0.18) if cuts else 1.0
    array = jax.random.normal(stream_key, dims, jnp.float32) * deviation * factor_of
    return jnp.minimum(jnp.maximum(array, -reach), reach).astype(dtype)


def setup_inputs(seed: int = 0) -> dict:
    splits = jax.random.split(jax.random.key(seed), 7)
    tokens = draw_tokens(jax.random.fold_in(splits[6], 71), 0)
    router = draw_router(jax.random.fold_in(splits[6], 71), 0)
    w_in = bell_draw(splits[2], (EXPERTS, D, HID), D ** -0.5, 0.15625, ((0, 128), (2, 2)))
    b_in = bell_draw(splits[3], (EXPERTS, HID), 0.5, 3.0, ((0, 128),))
    w_out = bell_draw(splits[4], (EXPERTS, HID, D), HID ** -0.5, 0.078125, ((0, 128), (1, 2)))
    b_out = bell_draw(splits[5], (EXPERTS, D), 0.5, 3.0, ((0, 128),))
    return {"tokens": tokens, "router": router, "w_in": w_in, "b_in": b_in, "w_out": w_out, "b_out": b_out}


def run_expert(packed):
    slot_rows, weight_in, bias_in, weight_out, bias_out = packed
    hidden = jax.nn.gelu(jnp.dot(slot_rows, weight_in, preferred_element_type=jnp.float32) + bias_in.astype(jnp.float32), approximate=False).astype(jnp.bfloat16)
    return (jnp.dot(hidden, weight_out, preferred_element_type=jnp.float32) + bias_out.astype(jnp.float32)).astype(jnp.bfloat16)


def reference(tokens, router, w_in, b_in, w_out, b_out):
    logits = jnp.einsum("bmd,de->bme", tokens.astype(jnp.float32), router.astype(jnp.float32))
    dispatch = jax.nn.softmax(logits, axis=1).astype(jnp.bfloat16)
    combine = jax.nn.softmax(logits, axis=2).astype(jnp.bfloat16)
    slots = jnp.einsum("bme,bmd->ebd", dispatch.astype(jnp.float32), tokens.astype(jnp.float32)).astype(jnp.bfloat16)
    expert_out = lax.map(run_expert, (slots, w_in, b_in, w_out, b_out))
    mixed = jnp.einsum("bme,ebd->bmd", combine.astype(jnp.float32), expert_out.astype(jnp.float32))
    return mixed.astype(jnp.bfloat16)
```

```python
import functools
import math

import jax
import jax.numpy as jnp
from jax import lax
from jax.experimental import pallas as pl
from jax.experimental.pallas import tpu as pltpu
from jax.sharding import Mesh
from jax.sharding import PartitionSpec as P

EXPERT = ("expert",)
ALL = ("dp", "expert")
CHUNK = 512


def front_kernel(x_hbm, r_hbm, slots_ref, comb_ref, x_ref, r_ref, sems):
    cx = pltpu.make_async_copy(x_hbm, x_ref, sems.at[0])
    cr = pltpu.make_async_copy(r_hbm, r_ref, sems.at[1])
    cx.start()
    cr.start()
    cx.wait()
    cr.wait()
    x = x_ref[...]
    logits = jnp.dot(x, r_ref[...], preferred_element_type=jnp.float32)
    top = jnp.max(logits, axis=0, keepdims=True)
    ex = jnp.exp(logits - top)
    dispatch = (ex / jnp.sum(ex, axis=0, keepdims=True)).astype(jnp.bfloat16)
    slots_ref[...] = lax.dot_general(
        dispatch, x, (((0,), (0,)), ((), ())), preferred_element_type=jnp.float32
    ).astype(jnp.bfloat16)
    top = jnp.max(logits, axis=1, keepdims=True)
    ex = jnp.exp(logits - top)
    comb_ref[...] = (ex / jnp.sum(ex, axis=1, keepdims=True)).astype(jnp.bfloat16)


def front(x, router):
    tokens, width = x.shape
    experts = router.shape[1]
    return pl.pallas_call(
        front_kernel,
        out_shape=(
            jax.ShapeDtypeStruct((experts, width), jnp.bfloat16),
            jax.ShapeDtypeStruct((tokens, experts), jnp.bfloat16),
        ),
        in_specs=[pl.BlockSpec(memory_space=pl.ANY)] * 2,
        out_specs=(pl.BlockSpec(memory_space=pltpu.VMEM),) * 2,
        scratch_shapes=[
            pltpu.VMEM(x.shape, x.dtype),
            pltpu.VMEM(router.shape, router.dtype),
            pltpu.SemaphoreType.DMA((2,)),
        ],
        name="front",
    )(x, router)


def mlp_kernel(x_ref, bi_ref, bo_ref, wi_hbm, wo_hbm, o_ref, wi, wo, acc, si, so):
    hid = wi.shape[1]
    n = hid // CHUNK
    half = lax.axis_index("dp")

    def copy_in(j):
        cols = pl.ds(j * CHUNK, CHUNK)
        return pltpu.make_async_copy(wi_hbm.at[:, cols], wi.at[:, cols], si.at[j])

    def copy_out(j):
        rows = pl.ds(j * CHUNK, CHUNK)
        return pltpu.make_async_copy(wo_hbm.at[rows, :], wo.at[rows, :], so.at[j])

    for j in range(n):
        copy_in(j).start()
        copy_out(j).start()
    bias = bi_ref[...].astype(jnp.float32)
    bias = jnp.where(half == 0, bias[:, :hid], bias[:, hid:])
    x = x_ref[...]

    def first(j):
        copy_in(j).wait()
        cols = pl.ds(j * CHUNK, CHUNK)
        return jnp.dot(x, wi[:, cols], preferred_element_type=jnp.float32)

    pre = first(0)
    for j in range(n):
        v = pre + bias[:, j * CHUNK : (j + 1) * CHUNK]
        if j + 1 < n:
            pre = first(j + 1)
        hidden = (v * (1.0 + lax.erf(v * (1.0 / math.sqrt(2.0)))) * 0.5).astype(jnp.bfloat16)
        copy_out(j).wait()
        part = jnp.dot(
            hidden, wo[pl.ds(j * CHUNK, CHUNK), :], preferred_element_type=jnp.float32
        )
        if j == 0:
            share = bo_ref[...].astype(jnp.float32)
            share = jnp.where(half == 0, share, jnp.zeros_like(share))
            acc[...] = part + share
        elif j + 1 < n:
            acc[...] += part
        else:
            o_ref[...] = (acc[...] + part).astype(jnp.bfloat16)


def mlp(x, w_in, b_in, w_out, b_out):
    rows, width = x.shape
    hid = w_in.shape[1]
    n = hid // CHUNK
    vmem = pl.BlockSpec(memory_space=pltpu.VMEM)
    hbm = pl.BlockSpec(memory_space=pl.ANY)
    return pl.pallas_call(
        mlp_kernel,
        out_shape=jax.ShapeDtypeStruct((rows, width), jnp.bfloat16),
        in_specs=[vmem, vmem, vmem, hbm, hbm],
        out_specs=vmem,
        scratch_shapes=[
            pltpu.VMEM(w_in.shape, w_in.dtype),
            pltpu.VMEM(w_out.shape, w_out.dtype),
            pltpu.VMEM((rows, width), jnp.float32),
            pltpu.SemaphoreType.DMA((n,)),
            pltpu.SemaphoreType.DMA((n,)),
        ],
        name="mlp",
    )(x, b_in, b_out, w_in, w_out)


def exchange(rows):
    count, width = rows.shape
    pieces = rows.reshape(count, 2, width // 2)
    pieces = lax.all_to_all(pieces, ALL, split_axis=0, concat_axis=0, tiled=True)
    return pieces.reshape(count, width)


def shards(tokens, router, w_in, b_in, w_out, b_out):
    slots, combine = front(tokens[0], router)
    arrived = exchange(jnp.concatenate([slots, slots], axis=0))
    share = mlp(arrived, w_in[0], b_in, w_out[0], b_out)
    returned = exchange(share)
    weights = jnp.concatenate([combine, combine], axis=1)
    mixed = jnp.dot(weights, returned, preferred_element_type=jnp.float32)
    return mixed.astype(jnp.bfloat16)[None]


def solution(mesh):
    return jax.shard_map(
        shards,
        mesh=mesh,
        in_specs=(
            P(ALL, None, None),
            P(),
            P("expert", None, "dp"),
            P("expert", None),
            P("expert", "dp", None),
            P("expert", None),
        ),
        out_specs=P(ALL, None, None),
        check_vma=False,
    )
```

```python
import functools
import math

import jax
import jax.numpy as jnp
from jax import lax
from jax.experimental import pallas as pl
from jax.experimental.pallas import tpu as pltpu
from jax.sharding import Mesh
from jax.sharding import PartitionSpec as P

EXPERT = ("expert",)
ALL = ("dp", "expert")
CHUNK = 512
AHEAD = CHUNK
FLIGHT = 4


def in_hbm(array):
    return pltpu.with_memory_space_constraint(array, pltpu.HBM)


def front_kernel(
    x_hbm, r_hbm, wi_hbm, bi_hbm, bo_hbm, slots_ref, comb_ref, ahead_ref, bias_ref, share_ref,
    x_ref, r_ref, bi_ref, bo_ref, sems,
):
    experts = r_ref.shape[1]
    half = lax.axis_index("dp")
    hid = bias_ref.shape[1]
    cx = pltpu.make_async_copy(x_hbm, x_ref, sems.at[0])
    cr = pltpu.make_async_copy(r_hbm, r_ref, sems.at[1])
    cw = pltpu.make_async_copy(wi_hbm.at[:, pl.ds(0, AHEAD)], ahead_ref, sems.at[2])
    ci = pltpu.make_async_copy(bi_hbm, bi_ref, sems.at[3])
    co = pltpu.make_async_copy(bo_hbm, bo_ref, sems.at[4])
    cx.start()
    cr.start()
    ci.start()
    co.start()
    cw.start()
    cx.wait()
    cr.wait()
    x = x_ref[...]
    logits = jnp.dot(x, r_ref[...], preferred_element_type=jnp.float32)
    top = jnp.max(logits, axis=0, keepdims=True)
    ex = jnp.exp(logits - top)
    dispatch = (ex / jnp.sum(ex, axis=0, keepdims=True)).astype(jnp.bfloat16)
    slots = lax.dot_general(
        dispatch, x, (((0,), (0,)), ((), ())), preferred_element_type=jnp.float32
    ).astype(jnp.bfloat16)
    slots_ref[:experts, :] = slots
    slots_ref[experts:, :] = slots
    top = jnp.max(logits, axis=1, keepdims=True)
    ex = jnp.exp(logits - top)
    combine = (ex / jnp.sum(ex, axis=1, keepdims=True)).astype(jnp.bfloat16)
    comb_ref[:, :experts] = combine
    comb_ref[:, experts:] = combine
    ci.wait()
    co.wait()
    bias = bi_ref[...].astype(jnp.float32)
    bias_ref[...] = jnp.where(half == 0, bias[:, :hid], bias[:, hid:])
    share = bo_ref[...].astype(jnp.float32)
    share_ref[...] = jnp.where(half == 0, share, jnp.zeros_like(share))
    cw.wait()


def front(x, router, w_in, b_in, b_out):
    tokens, width = x.shape
    experts = router.shape[1]
    return pl.pallas_call(
        front_kernel,
        out_shape=(
            jax.ShapeDtypeStruct((2 * experts, width), jnp.bfloat16),
            jax.ShapeDtypeStruct((tokens, 2 * experts), jnp.bfloat16),
            jax.ShapeDtypeStruct((width, AHEAD), jnp.bfloat16),
            jax.ShapeDtypeStruct((1, w_in.shape[1]), jnp.float32),
            jax.ShapeDtypeStruct(b_out.shape, jnp.float32),
        ),
        in_specs=[pl.BlockSpec(memory_space=pltpu.HBM)] * 5,
        out_specs=(pl.BlockSpec(memory_space=pltpu.VMEM),) * 5,
        scratch_shapes=[
            pltpu.VMEM(x.shape, x.dtype),
            pltpu.VMEM(router.shape, router.dtype),
            pltpu.VMEM(b_in.shape, b_in.dtype),
            pltpu.VMEM(b_out.shape, b_out.dtype),
            pltpu.SemaphoreType.DMA((5,)),
        ],
        compiler_params=pltpu.CompilerParams(vmem_limit_bytes=8 << 20),
        name="front",
    )(in_hbm(x), in_hbm(router), in_hbm(w_in), in_hbm(b_in), in_hbm(b_out))


def mlp_kernel(x_ref, ahead_ref, bias_ref, share_ref, wi_hbm, wo_hbm, o_ref, wi, wo, acc, si, so):
    n = wi.shape[1] // CHUNK

    def copy_in(j):
        cols = pl.ds(j * CHUNK, CHUNK)
        return pltpu.make_async_copy(wi_hbm.at[:, cols], wi.at[:, cols], si.at[j])

    def copy_out(j):
        rows = pl.ds(j * CHUNK, CHUNK)
        return pltpu.make_async_copy(wo_hbm.at[rows, :], wo.at[rows, :], so.at[j])

    copies = [copy_out(0)]
    for j in range(1, n):
        copies += [copy_in(j), copy_out(j)]
    for copy in copies[:FLIGHT]:
        copy.start()

    def wait(k):
        copies[k].wait()
        if k + FLIGHT < len(copies):
            copies[k + FLIGHT].start()

    x = x_ref[...]
    pre = jnp.dot(x, ahead_ref[...], preferred_element_type=jnp.float32)
    for j in range(n):
        cols = pl.ds(j * CHUNK, CHUNK)
        v = pre + bias_ref[:, cols]
        hidden = (v * (1.0 + lax.erf(v * (1.0 / math.sqrt(2.0)))) * 0.5).astype(jnp.bfloat16)
        wait(2 * j)
        if j + 1 < n:
            wait(2 * j + 1)
            pre = jnp.dot(
                x, wi[:, pl.ds((j + 1) * CHUNK, CHUNK)], preferred_element_type=jnp.float32
            )
        part = jnp.dot(hidden, wo[cols, :], preferred_element_type=jnp.float32)
        if j == 0:
            acc[...] = part + share_ref[...]
        elif j + 1 < n:
            acc[...] += part
        else:
            o_ref[...] = (acc[...] + part).astype(jnp.bfloat16)


def mlp(x, ahead, bias, share, w_in, w_out):
    rows, width = x.shape
    n = w_in.shape[1] // CHUNK
    vmem = pl.BlockSpec(memory_space=pltpu.VMEM)
    hbm = pl.BlockSpec(memory_space=pltpu.HBM)
    return pl.pallas_call(
        mlp_kernel,
        out_shape=jax.ShapeDtypeStruct((rows, width), jnp.bfloat16),
        in_specs=[vmem, vmem, vmem, vmem, hbm, hbm],
        out_specs=vmem,
        scratch_shapes=[
            pltpu.VMEM(w_in.shape, w_in.dtype),
            pltpu.VMEM(w_out.shape, w_out.dtype),
            pltpu.VMEM((rows, width), jnp.float32),
            pltpu.SemaphoreType.DMA((n,)),
            pltpu.SemaphoreType.DMA((n,)),
        ],
        compiler_params=pltpu.CompilerParams(vmem_limit_bytes=24 << 20),
        name="mlp",
    )(x, ahead, bias, share, in_hbm(w_in), in_hbm(w_out))


def exchange(rows):
    count, width = rows.shape
    pieces = rows.reshape(count, 2, width // 2)
    pieces = lax.all_to_all(pieces, ALL, split_axis=0, concat_axis=0, tiled=True)
    return pieces.reshape(count, width)


def shards(tokens, router, w_in, b_in, w_out, b_out):
    slots, weights, ahead, bias, share = front(tokens[0], router, w_in[0], b_in, b_out)
    arrived = exchange(slots)
    share = mlp(arrived, ahead, bias, share, w_in[0], w_out[0])
    returned = exchange(share)
    mixed = jnp.dot(weights, returned, preferred_element_type=jnp.float32)
    return mixed.astype(jnp.bfloat16)[None]


def solution(mesh):
    return jax.shard_map(
        shards,
        mesh=mesh,
        in_specs=(
            P(ALL, None, None),
            P(),
            P("expert", None, "dp"),
            P("expert", None),
            P("expert", "dp", None),
            P("expert", None),
        ),
        out_specs=P(ALL, None, None),
        check_vma=False,
    )
```

```python
import functools
import math

import jax
import jax.numpy as jnp
from jax import lax
from jax.experimental import pallas as pl
from jax.experimental.pallas import tpu as pltpu
from jax.sharding import Mesh
from jax.sharding import PartitionSpec as P

EXPERT = ("expert",)
ALL = ("dp", "expert")
CHUNK = 512
GRANT = 8 << 20
PARTS = 2
HOLD_FLOPS = 20_000_000_000
HOLD_BYTES = 64 << 20


def in_hbm(array):
    return pltpu.with_memory_space_constraint(array, pltpu.HBM)


def front_kernel(
    x_hbm, r_hbm, bi_hbm, bo_hbm, slots_ref, comb_ref, bias_ref, share_ref,
    x_ref, r_ref, bi_ref, bo_ref, sems,
):
    experts = r_ref.shape[1]
    half = lax.axis_index("dp")
    hid = bias_ref.shape[1]
    cx = pltpu.make_async_copy(x_hbm, x_ref, sems.at[0])
    cr = pltpu.make_async_copy(r_hbm, r_ref, sems.at[1])
    ci = pltpu.make_async_copy(bi_hbm, bi_ref, sems.at[2])
    co = pltpu.make_async_copy(bo_hbm, bo_ref, sems.at[3])
    cx.start()
    cr.start()
    ci.start()
    co.start()
    cx.wait()
    cr.wait()
    x = x_ref[...]
    logits = jnp.dot(x, r_ref[...], preferred_element_type=jnp.float32)
    top = jnp.max(logits, axis=0, keepdims=True)
    ex = jnp.exp(logits - top)
    dispatch = (ex / jnp.sum(ex, axis=0, keepdims=True)).astype(jnp.bfloat16)
    slots = lax.dot_general(
        dispatch, x, (((0,), (0,)), ((), ())), preferred_element_type=jnp.float32
    )
    width = slots.shape[1]
    slots = slots.astype(jnp.bfloat16).reshape(experts, 2, width // 2)
    slots_ref[:experts] = slots
    slots_ref[experts:] = slots
    top = jnp.max(logits, axis=1, keepdims=True)
    ex = jnp.exp(logits - top)
    combine = (ex / jnp.sum(ex, axis=1, keepdims=True)).astype(jnp.bfloat16)
    comb_ref[:, :experts] = combine
    comb_ref[:, experts:] = combine
    ci.wait()
    co.wait()
    bias = bi_ref[...].astype(jnp.float32)
    bias_ref[...] = jnp.where(half == 0, bias[:, :hid], bias[:, hid:])
    share = bo_ref[...].astype(jnp.float32)
    share_ref[...] = jnp.where(half == 0, share, jnp.zeros_like(share))


def front(x, router, b_in, b_out, hid):
    tokens, width = x.shape
    experts = router.shape[1]
    return pl.pallas_call(
        front_kernel,
        out_shape=(
            jax.ShapeDtypeStruct((2 * experts, 2, width // 2), jnp.bfloat16),
            jax.ShapeDtypeStruct((tokens, 2 * experts), jnp.bfloat16),
            jax.ShapeDtypeStruct((1, hid), jnp.float32),
            jax.ShapeDtypeStruct(b_out.shape, jnp.float32),
        ),
        in_specs=[pl.BlockSpec(memory_space=pltpu.HBM)] * 4,
        out_specs=(pl.BlockSpec(memory_space=pltpu.VMEM),) * 4,
        scratch_shapes=[
            pltpu.VMEM(x.shape, x.dtype),
            pltpu.VMEM(router.shape, router.dtype),
            pltpu.VMEM(b_in.shape, b_in.dtype),
            pltpu.VMEM(b_out.shape, b_out.dtype),
            pltpu.SemaphoreType.DMA((4,)),
        ],
        compiler_params=pltpu.CompilerParams(vmem_limit_bytes=8 << 20),
        name="front",
    )(in_hbm(x), in_hbm(router), in_hbm(b_in), in_hbm(b_out))


def mlp_kernel(x_ref, bias_ref, share_ref, wi, wo, o_ref, hid):
    x = x_ref[...]
    for j in range(wi.shape[1] // CHUNK):
        cols = pl.ds(j * CHUNK, CHUNK)
        v = jnp.dot(x, wi[:, cols], preferred_element_type=jnp.float32) + bias_ref[:, cols]
        hid[:, cols] = (v * (1.0 + lax.erf(v * (1.0 / math.sqrt(2.0)))) * 0.5).astype(jnp.bfloat16)
    part = jnp.dot(hid[...], wo[...], preferred_element_type=jnp.float32)
    o_ref[...] = (part + share_ref[...]).astype(jnp.bfloat16)


def mlp(x, bias, share, w_in, w_out):
    rows, width = x.shape
    vmem = pl.BlockSpec(memory_space=pltpu.VMEM)
    return pl.pallas_call(
        mlp_kernel,
        out_shape=jax.ShapeDtypeStruct((rows, width), jnp.bfloat16),
        in_specs=[vmem] * 5,
        out_specs=vmem,
        scratch_shapes=[pltpu.VMEM((rows, w_in.shape[1]), jnp.bfloat16)],
        compiler_params=pltpu.CompilerParams(vmem_limit_bytes=GRANT),
        name="mlp",
    )(x, bias, share, w_in, w_out)


def hold_kernel(x_ref, o_ref):
    pass


def hold(x):
    vmem = pl.BlockSpec(memory_space=pltpu.VMEM)
    return pl.pallas_call(
        hold_kernel,
        out_shape=jax.ShapeDtypeStruct(x.shape, x.dtype),
        in_specs=[vmem],
        out_specs=vmem,
        input_output_aliases={0: 0},
        compiler_params=pltpu.CompilerParams(vmem_limit_bytes=1 << 20),
        cost_estimate=pl.CostEstimate(
            flops=HOLD_FLOPS, bytes_accessed=HOLD_BYTES, transcendentals=0
        ),
        name="hold",
    )(x)


def mix_kernel(w_ref, r_ref, o_hbm, out, sems):
    rows = out.shape[0] // PARTS
    copies = []
    for i in range(PARTS):
        part = pl.ds(i * rows, rows)
        out[part, :] = jnp.dot(
            w_ref[part, :], r_ref[...], preferred_element_type=jnp.float32
        ).astype(jnp.bfloat16)
        copies.append(pltpu.make_async_copy(out.at[part, :], o_hbm.at[part, :], sems.at[i]))
        copies[-1].start()
    for copy in copies:
        copy.wait()


def mix(weights, returned):
    shape = (weights.shape[0], returned.shape[1])
    vmem = pl.BlockSpec(memory_space=pltpu.VMEM)
    return pl.pallas_call(
        mix_kernel,
        out_shape=jax.ShapeDtypeStruct(shape, jnp.bfloat16),
        in_specs=[vmem, vmem],
        out_specs=pl.BlockSpec(memory_space=pltpu.HBM),
        scratch_shapes=[pltpu.VMEM(shape, jnp.bfloat16), pltpu.SemaphoreType.DMA((PARTS,))],
        compiler_params=pltpu.CompilerParams(vmem_limit_bytes=8 << 20),
        name="mix",
    )(weights, returned)


def exchange(pieces):
    count = pieces.shape[0]
    pieces = lax.all_to_all(pieces, ALL, split_axis=0, concat_axis=0, tiled=True)
    return pieces.reshape(count, -1)


def shards(tokens, router, w_in, b_in, w_out, b_out):
    slots, weights, bias, share = front(tokens[0], router, b_in, b_out, w_in.shape[2])
    arrived = exchange(hold(hold(slots)))
    share = mlp(arrived, bias, share, w_in[0], w_out[0])
    returned = exchange(share.reshape(share.shape[0], 2, -1))
    return mix(weights, returned)[None]


def solution(mesh):
    return jax.shard_map(
        shards,
        mesh=mesh,
        in_specs=(
            P(ALL, None, None),
            P(),
            P("expert", None, "dp"),
            P("expert", None),
            P("expert", "dp", None),
            P("expert", None),
        ),
        out_specs=P(ALL, None, None),
        check_vma=False,
    )
```

```python
import functools
import math

import jax
import jax.numpy as jnp
from jax import lax
from jax.experimental import pallas as pl
from jax.experimental.pallas import tpu as pltpu
from jax.sharding import Mesh
from jax.sharding import PartitionSpec as P

EXPERT = ("expert",)
ALL = ("dp", "expert")
CHUNK = 1280
GRANT = 8 << 20
PARTS = 2
HOLD_FLOPS = 20_000_000_000
HOLD_BYTES = 64 << 20


def in_hbm(array):
    return pltpu.with_memory_space_constraint(array, pltpu.HBM)


def front_kernel(
    x_hbm, r_hbm, bi_hbm, bo_hbm, slots_ref, comb_ref, bias_ref, share_ref,
    x_ref, r_ref, bi_ref, bo_ref, sems,
):
    experts = r_ref.shape[1]
    half = lax.axis_index("dp")
    hid = bias_ref.shape[1]
    cx = pltpu.make_async_copy(x_hbm, x_ref, sems.at[0])
    cr = pltpu.make_async_copy(r_hbm, r_ref, sems.at[1])
    ci = pltpu.make_async_copy(bi_hbm, bi_ref, sems.at[2])
    co = pltpu.make_async_copy(bo_hbm, bo_ref, sems.at[3])
    cx.start()
    cr.start()
    ci.start()
    co.start()
    ci.wait()
    co.wait()
    bias = bi_ref[...].astype(jnp.float32)
    bias_ref[...] = jnp.where(half == 0, bias[:, :hid], bias[:, hid:])
    share = bo_ref[...].astype(jnp.float32)
    share_ref[...] = jnp.where(half == 0, share, jnp.zeros_like(share))
    cx.wait()
    cr.wait()
    x = x_ref[...]
    logits = jnp.dot(x, r_ref[...], preferred_element_type=jnp.float32)
    top = jnp.max(logits, axis=0, keepdims=True)
    ex = jnp.exp(logits - top)
    dispatch = (ex / jnp.sum(ex, axis=0, keepdims=True)).astype(jnp.bfloat16)
    slots = lax.dot_general(
        dispatch, x, (((0,), (0,)), ((), ())), preferred_element_type=jnp.float32
    )
    width = slots.shape[1]
    slots = slots.astype(jnp.bfloat16).reshape(experts, 2, width // 2)
    slots_ref[:experts] = slots
    slots_ref[experts:] = slots
    top = jnp.max(logits, axis=1, keepdims=True)
    ex = jnp.exp(logits - top)
    combine = (ex / jnp.sum(ex, axis=1, keepdims=True)).astype(jnp.bfloat16)
    comb_ref[:, :experts] = combine
    comb_ref[:, experts:] = combine


def front(x, router, b_in, b_out, hid):
    tokens, width = x.shape
    experts = router.shape[1]
    return pl.pallas_call(
        front_kernel,
        out_shape=(
            jax.ShapeDtypeStruct((2 * experts, 2, width // 2), jnp.bfloat16),
            jax.ShapeDtypeStruct((tokens, 2 * experts), jnp.bfloat16),
            jax.ShapeDtypeStruct((1, hid), jnp.float32),
            jax.ShapeDtypeStruct(b_out.shape, jnp.float32),
        ),
        in_specs=[pl.BlockSpec(memory_space=pltpu.HBM)] * 4,
        out_specs=(pl.BlockSpec(memory_space=pltpu.VMEM),) * 4,
        scratch_shapes=[
            pltpu.VMEM(x.shape, x.dtype),
            pltpu.VMEM(router.shape, router.dtype),
            pltpu.VMEM(b_in.shape, b_in.dtype),
            pltpu.VMEM(b_out.shape, b_out.dtype),
            pltpu.SemaphoreType.DMA((4,)),
        ],
        compiler_params=pltpu.CompilerParams(vmem_limit_bytes=8 << 20),
        name="front",
    )(in_hbm(x), in_hbm(router), in_hbm(b_in), in_hbm(b_out))


def mlp_kernel(x_ref, bias_ref, share_ref, wi, wo, o_ref, hid):
    x = x_ref[...]
    for j in range(wi.shape[1] // CHUNK):
        cols = pl.ds(j * CHUNK, CHUNK)
        v = jnp.dot(x, wi[:, cols], preferred_element_type=jnp.float32) + bias_ref[:, cols]
        hid[:, cols] = (v * (1.0 + lax.erf(v * (1.0 / math.sqrt(2.0)))) * 0.5).astype(jnp.bfloat16)
    part = jnp.dot(hid[...], wo[...], preferred_element_type=jnp.float32)
    o_ref[...] = (part + share_ref[...]).astype(jnp.bfloat16)


def mlp(x, bias, share, w_in, w_out):
    rows, width = x.shape
    vmem = pl.BlockSpec(memory_space=pltpu.VMEM)
    return pl.pallas_call(
        mlp_kernel,
        out_shape=jax.ShapeDtypeStruct((rows, width), jnp.bfloat16),
        in_specs=[vmem] * 5,
        out_specs=vmem,
        scratch_shapes=[pltpu.VMEM((rows, w_in.shape[1]), jnp.bfloat16)],
        compiler_params=pltpu.CompilerParams(vmem_limit_bytes=GRANT),
        name="mlp",
    )(x, bias, share, w_in, w_out)


def hold_kernel(x_ref, o_ref):
    pass


def hold(x):
    vmem = pl.BlockSpec(memory_space=pltpu.VMEM)
    return pl.pallas_call(
        hold_kernel,
        out_shape=jax.ShapeDtypeStruct(x.shape, x.dtype),
        in_specs=[vmem],
        out_specs=vmem,
        input_output_aliases={0: 0},
        compiler_params=pltpu.CompilerParams(vmem_limit_bytes=1 << 20),
        cost_estimate=pl.CostEstimate(
            flops=HOLD_FLOPS, bytes_accessed=HOLD_BYTES, transcendentals=0
        ),
        name="hold",
    )(x)


def mix_kernel(w_ref, r_ref, o_hbm, out, sems):
    rows = out.shape[0] // PARTS
    copies = []
    for i in range(PARTS):
        part = pl.ds(i * rows, rows)
        out[part, :] = jnp.dot(
            w_ref[part, :], r_ref[...], preferred_element_type=jnp.float32
        ).astype(jnp.bfloat16)
        copies.append(pltpu.make_async_copy(out.at[part, :], o_hbm.at[part, :], sems.at[i]))
        copies[-1].start()
    for copy in copies:
        copy.wait()


def mix(weights, returned):
    shape = (weights.shape[0], returned.shape[1])
    vmem = pl.BlockSpec(memory_space=pltpu.VMEM)
    return pl.pallas_call(
        mix_kernel,
        out_shape=jax.ShapeDtypeStruct(shape, jnp.bfloat16),
        in_specs=[vmem, vmem],
        out_specs=pl.BlockSpec(memory_space=pltpu.HBM),
        scratch_shapes=[pltpu.VMEM(shape, jnp.bfloat16), pltpu.SemaphoreType.DMA((PARTS,))],
        compiler_params=pltpu.CompilerParams(vmem_limit_bytes=8 << 20),
        name="mix",
    )(weights, returned)


def exchange(pieces):
    count = pieces.shape[0]
    pieces = lax.all_to_all(pieces, ALL, split_axis=0, concat_axis=0, tiled=True)
    return pieces.reshape(count, -1)


def shards(tokens, router, w_in, b_in, w_out, b_out):
    slots, weights, bias, share = front(tokens[0], router, b_in, b_out, w_in.shape[2])
    arrived = exchange(hold(hold(slots)))
    share = mlp(arrived, bias, share, w_in[0], w_out[0])
    returned = exchange(share.reshape(share.shape[0], 2, -1))
    return mix(weights, returned)[None]


def solution(mesh):
    return jax.shard_map(
        shards,
        mesh=mesh,
        in_specs=(
            P(ALL, None, None),
            P(),
            P("expert", None, "dp"),
            P("expert", None),
            P("expert", "dp", None),
            P("expert", None),
        ),
        out_specs=P(ALL, None, None),
        check_vma=False,
    )
```
